32 devices in a mesh: seq: 8 (over z, x), head: 4 (over y, core).
Axes of the slice: x: 2, y: 2, z: 4, core: 2. Of those that a mesh axis runs over, the one named last changes fastest.
Arguments:
- queries: bfloat16 [2048, 4096], P('seq', 'head'), may hold values from -48 to 48
- key_rows: bfloat16 [2048, 4096], P('seq', 'head'), may hold values from -4 to 4
- value_rows: bfloat16 [2048, 4096], P('seq', 'head'), may hold values from -6 to 6
- out_grad: bfloat16 [2048, 2048], P('seq', 'head'), may hold values from -6 to 6
- out_proj: bfloat16 [4096, 2048], P('head'), may hold values from -0.125 to 0.125
- section_table: int32 [32, 3], P('head'), may hold values 0 or 1
- block_active: int32 [8, 3], P('seq'), may hold values 0 or 1
Outputs:
- query_grad: bfloat16 [2048, 4096], P('seq', 'head')
- key_grad: bfloat16 [2048, 4096], P('seq', 'head')
- value_grad: bfloat16 [2048, 4096], P('seq', 'head')
The draws below stay inside these ranges and needn't reach their ends.
All inputs are finite; a program needn't handle non-finite values.
Results may differ from the reference program's by a relative error of at most 0.008.
Values may be sent and summed in bfloat16 or wider, within the bound.
A program may use at most 64 MiB of HBM per device.

```python
import math
from functools import partial
from functools import reduce
import jax
import jax.numpy as jnp
from jax import lax

BLK = 256
HEADS = 32
HDIM = 128
DMODEL = 2048
SECTIONS = 3
NBLOCKS = 8
TOKENS = 2048


def paired_fields(key):
    base_key = jax.random.fold_in(key, 4021)
    field_shape = (TOKENS, HEADS * HDIM)
    key_field = jnp.clip(jax.random.normal(jax.random.fold_in(base_key, 1), field_shape, jnp.float32), -4.0, 4.0)
    query_field = jnp.clip(jax.random.normal(jax.random.fold_in(base_key, 2), field_shape, jnp.float32), -4.0, 4.0)
    return (query_field, key_field)


def draw_queries(key, part):
    return paired_fields(key)[0].astype(jnp.bfloat16)


def draw_key_rows(key, part):
    return paired_fields(key)[1].astype(jnp.bfloat16)


def plant(values, key, smallest, top_value):
    shape = values.shape
    spot = [jax.random.randint(jax.random.fold_in(key, axis), (), 0, shape[axis]) for axis in range(len(shape))]
    values = values.at[tuple(spot)].set(smallest)
    longest = shape.index(max(shape))
    spot[longest] = (spot[longest] + 1) % shape[longest]
    return values.at[tuple(spot)].set(top_value)


def steps_of(rng, shape, shards, smallest, largest):
    factor_of, own = 1.0, jax.random.fold_in(rng, 6)
    for dim, shards_of in shards:
        heights = jnp.exp(jax.random.uniform(jax.random.fold_in(own, dim), (shards_of,), jnp.float32, smallest / len(shards), largest / len(shards)))
        factor_of = factor_of * jnp.repeat(heights, shape[dim] // shards_of).reshape([-1 if axis == dim else 1 for axis in range(len(shape))])
    return factor_of


def centred(own_key, dims, width, bound, split=(), held_as=jnp.bfloat16):
    drawn = width * jax.random.normal(own_key, dims, jnp.float32)
    if split:
        drawn = drawn * steps_of(own_key, dims, split, -0.22, 0.18)
    return jnp.clip(drawn, -bound, bound).astype(held_as)


def setup_inputs(seed: int = 0) -> dict:
    key_list = jax.random.split(jax.random.key(seed), 8)
    return {
        "queries": draw_queries(jax.random.fold_in(key_list[7], 71), 0),
        "key_rows": draw_key_rows(jax.random.fold_in(key_list[7], 71), 0),
        "value_rows": centred(key_list[2], (TOKENS, HEADS * HDIM), 1.0, 6.0, ((0, 8), (1, 4))),
        "out_grad": centred(key_list[3], (TOKENS, DMODEL), 1.0, 6.0, ((0, 8), (1, 4))),
        "out_proj": centred(key_list[4], (HEADS * HDIM, DMODEL), DMODEL ** -0.5, 0.125, ((0, 4),)),
        "section_table": plant((jax.random.randint(key_list[5], (HEADS, SECTIONS), 0, 3) < 2).astype(jnp.int32), jax.random.fold_in(key_list[5], 1), 0, 1),
        "block_active": plant((jax.random.randint(key_list[6], (NBLOCKS, SECTIONS), 0, 4) < 3).astype(jnp.int32), jax.random.fold_in(key_list[6], 1), 0, 1),
    }


def shift_down(blocks, count):
    filler = jnp.zeros((count,) + blocks.shape[1:], blocks.dtype)
    return jnp.concatenate([filler, blocks[:blocks.shape[0] - count]], axis=0)

def shift_up(blocks, count):
    filler = jnp.zeros((count,) + blocks.shape[1:], blocks.dtype)
    return jnp.concatenate([blocks[count:], filler], axis=0)

def to_wide(array):
    return array.astype(jnp.float32)

def narrow(array):
    return lax.optimization_barrier(array.astype(jnp.bfloat16)).astype(jnp.float32)

def head_grads(block_active, operands):
    query_h, key_h, value_h, grad_h, head_flags = operands
    score_scale = 1.0 / math.sqrt(HDIM)
    query_wide = to_wide(query_h)
    key_wide = to_wide(key_h)
    value_wide = to_wide(value_h)
    grad_wide = to_wide(grad_h)
    row_ids = jnp.arange(BLK)
    causal = (row_ids[:, None] >= row_ids[None, :])[None]
    block_ids = jnp.arange(NBLOCKS)
    key_sets = [(key_wide, value_wide, causal, 0)]
    for section_index in range(SECTIONS):
        shift_count = NBLOCKS // 2 ** (section_index + 1)
        usable = (head_flags[section_index] * block_active[:, section_index] > 0) & (block_ids >= shift_count)
        key_sets.append((shift_down(key_wide, shift_count), shift_down(value_wide, shift_count), usable[:, None, None], shift_count))
    logits = []
    for key_entry in key_sets:
        raw_scores = jnp.einsum('bid,bjd->bij', query_wide, key_entry[0]) * score_scale
        logits.append(jnp.where(key_entry[2], raw_scores, -1e+30))
    row_max = reduce(jnp.maximum, [lax.optimization_barrier(jnp.max(logit_set, axis=-1)) for logit_set in logits])
    row_sum = reduce(jnp.add, [lax.optimization_barrier(jnp.sum(jnp.exp(logit_set - row_max[..., None]), axis=-1)) for logit_set in logits])
    log_norm = row_max + jnp.log(row_sum)
    probs_list = [jnp.where(key_entry[2], jnp.exp(logit_set - log_norm[..., None]), 0.0) for logit_set, key_entry in zip(logits, key_sets)]
    weight_list = [narrow(prob_set) for prob_set in probs_list]
    context = reduce(jnp.add, [jnp.einsum('bij,bjd->bid', weight_set, key_entry[1]) for weight_set, key_entry in zip(weight_list, key_sets)])
    row_delta = lax.optimization_barrier(jnp.sum(grad_wide * context, axis=-1))
    query_grad = jnp.zeros_like(query_wide)
    key_grad = jnp.zeros_like(query_wide)
    value_grad = jnp.zeros_like(query_wide)
    for set_index in range(SECTIONS + 1):
        key_part, value_part, allowed, shift_count = key_sets[set_index]
        prob_grad = jnp.einsum('bid,bjd->bij', grad_wide, value_part)
        dlogit = narrow(probs_list[set_index] * (prob_grad - row_delta[..., None]) * score_scale)
        query_grad = query_grad + jnp.einsum('bij,bjd->bid', dlogit, key_part)
        key_term = jnp.einsum('bij,bid->bjd', dlogit, query_wide)
        value_term = jnp.einsum('bij,bid->bjd', weight_list[set_index], grad_wide)
        if set_index > 0:
            key_term = narrow(key_term)
            value_term = narrow(value_term)
        key_grad = key_grad + shift_up(key_term, shift_count)
        value_grad = value_grad + shift_up(value_term, shift_count)
    return (query_grad.astype(jnp.bfloat16), key_grad.astype(jnp.bfloat16), value_grad.astype(jnp.bfloat16))

def by_heads(matrix):
    return matrix.reshape(NBLOCKS, BLK, HEADS, HDIM).transpose(2, 0, 1, 3)

def from_heads(stacked):
    return stacked.transpose(1, 2, 0, 3).reshape(TOKENS, HEADS * HDIM)

def reference(queries, key_rows, value_rows, out_grad, out_proj, section_table, block_active):
    attn_grad = jnp.dot(out_grad, out_proj.T, preferred_element_type=jnp.float32).astype(jnp.bfloat16)
    operands = (by_heads(queries), by_heads(key_rows), by_heads(value_rows), by_heads(attn_grad), section_table)
    query_out, key_out, value_out = lax.map(partial(head_grads, block_active), operands)
    return (from_heads(query_out), from_heads(key_out), from_heads(value_out))
```

```python
import functools
import math

import jax
import jax.numpy as jnp
from jax import lax
from jax.experimental import pallas as pl
from jax.experimental.pallas import tpu as pltpu
from jax.sharding import PartitionSpec as P

HDIM = 128
SECTIONS = 3
AHEAD = 2
MESH = pl.DeviceIdType.MESH
BF16 = jnp.bfloat16
F32 = jnp.float32


def dot(a, b, dims):
    return lax.dot_general(a, b, (dims, ((), ())), preferred_element_type=F32)


def kernel(
    count,
    lanes,
    q_ref,
    k_hbm,
    v_hbm,
    og_hbm,
    proj_hbm,
    table_ref,
    active_ref,
    dq_ref,
    dk_ref,
    dv_ref,
    kv,
    reach,
    term,
    back,
    own,
    og,
    proj,
    local_sem,
    load_sem,
    og_send,
    og_recv,
    fwd_send,
    fwd_recv,
    bwd_send,
    bwd_recv,
):
    heads, _, rows, _ = kv.shape
    width = og.shape[2]
    scale = 1.0 / math.sqrt(HDIM)
    quarter, eighth = count // 4, count // 8
    me = lax.axis_index("seq")
    lane = lax.axis_index("head")
    odd = (me // eighth) % 2 == 1
    even = jnp.logical_not(odd)
    up, down = me + quarter, me - quarter
    pair = jnp.where(odd, me - eighth, me + eighth)
    has_up, has_down = me < count - quarter, me >= quarter
    has_far = me >= 2 * quarter
    has_both = jnp.logical_and(has_up, has_down)
    odd_or_down = jnp.logical_or(odd, has_down)
    even_or_down = jnp.logical_or(even, has_down)
    twin = jnp.where(lane % 2 == 1, lane - 1, lane + 1)

    def cols(c):
        return pl.ds(pl.multiple_of(c * HDIM, HDIM), HDIM)

    def remote(src, dst, send, recv, axis, target):
        return pltpu.make_async_remote_copy(
            src_ref=src,
            dst_ref=dst,
            send_sem=send,
            recv_sem=recv,
            device_id={axis: target},
            device_id_type=MESH,
        )

    def fwd(kind, src, c, target):
        return remote(
            src.at[c], reach.at[kind, c], fwd_send.at[kind, c], fwd_recv.at[kind, c], "seq", target
        )

    def bwd(kind, c, target):
        return remote(
            term.at[kind, c],
            back.at[kind, c],
            bwd_send.at[kind, c],
            bwd_recv.at[kind, c],
            "seq",
            target,
        )

    def load_kv(c):
        return [
            pltpu.make_async_copy(src.at[:, cols(c)], kv.at[c, j], local_sem.at[j, c])
            for j, src in enumerate((k_hbm, v_hbm))
        ]

    load_og = pltpu.make_async_copy(og_hbm, og.at[lane], load_sem.at[0])
    load_proj = pltpu.make_async_copy(proj_hbm, proj, load_sem.at[1])
    load_og.start()

    @pl.loop(0, heads)
    def _(c):
        for copy in load_kv(c):
            copy.start()

    load_proj.start()

    barrier = pltpu.get_barrier_semaphore()
    peers = [lax.rem(lane + 2 * j, lanes) for j in range(1, lanes // 2)]
    for peer in [twin] + peers:
        pl.semaphore_signal(barrier, inc=1, device_id={"head": peer}, device_id_type=MESH)
    pl.semaphore_signal(barrier, inc=1, device_id={"seq": pair}, device_id_type=MESH)

    @pl.when(has_up)
    def _():
        pl.semaphore_signal(barrier, inc=1, device_id={"seq": up}, device_id_type=MESH)

    @pl.when(has_down)
    def _():
        pl.semaphore_signal(barrier, inc=1, device_id={"seq": down}, device_id_type=MESH)

    pl.semaphore_wait(
        barrier, 2 + len(peers) + has_up.astype(jnp.int32) + has_down.astype(jnp.int32)
    )

    def send_own(c):
        for copy in load_kv(c):
            copy.wait()

        @pl.when(has_up)
        def _():
            fwd(1, kv, c, up).start()

        @pl.when(even)
        def _():
            fwd(2, kv, c, pair).start()

    def forward(c):
        @pl.when(has_down)
        def _():
            fwd(1, kv, c, up).wait_recv()

        @pl.when(has_both)
        def _():
            fwd(0, reach.at[1], c, up).start()

        @pl.when(jnp.logical_and(odd, has_down))
        def _():
            fwd(2, reach.at[1], c, pair).start()

        @pl.when(c + AHEAD < heads)
        def _():
            send_own(c + AHEAD)

    def og_peer(index, slot, target):
        return remote(
            og.at[slot], og.at[slot], og_send.at[index], og_recv.at[slot], "head", target
        )

    load_og.wait()
    for j, peer in enumerate(peers):
        og_peer(1 + j, lane, peer).start()
    og_peer(0, lane, twin).start()
    for c in range(AHEAD):
        send_own(jnp.int32(c))

    for present, buffer in (
        (has_far, reach.at[0]),
        (has_down, reach.at[1]),
        (odd_or_down, reach.at[2]),
        (has_both, back.at[0]),
        (has_up, back.at[1]),
        (even_or_down, back.at[2]),
    ):

        @pl.when(jnp.logical_not(present))
        def _():
            @pl.loop(0, heads)
            def _(c):
                buffer[c] = jnp.zeros(buffer.shape[1:], BF16)

    forward(jnp.int32(0))
    for j, peer in enumerate(peers):
        og_peer(1 + j, peer, lane).wait_recv()
        og_peer(len(peers) + 1 + j, peer, twin).start()
    load_proj.wait()
    og_peer(0, twin, lane).wait_recv()
    for j in range(len(peers)):
        og_peer(len(peers) + 1 + j, lax.rem(twin + 2 * (j + 1), lanes), lane).wait_recv()

    key_index = lax.broadcasted_iota(jnp.int32, (rows, rows), 0)
    query_index = lax.broadcasted_iota(jnp.int32, (rows, rows), 1)

    def compute(c):
        grad = sum(
            dot(og[p], proj[cols(c), p * width : (p + 1) * width], ((1,), (1,)))
            for p in range(lanes)
        ).astype(BF16)
        query = q_ref[:, cols(c)]

        @pl.when(has_far)
        def _():
            fwd(0, kv, c, up).wait_recv()

        @pl.when(odd_or_down)
        def _():
            fwd(2, kv, c, pair).wait_recv()

        pieces = [(kv[c, 0], kv[c, 1])] + [
            (reach[k, c, 0], reach[k, c, 1]) for k in range(SECTIONS)
        ]
        logits = []
        for k, (key, _) in enumerate(pieces):
            raw = dot(key, query, ((1,), (1,))) * scale
            if k == 0:
                raw = jnp.where(key_index <= query_index, raw, -1e30)
            else:
                usable = jnp.logical_and(
                    table_ref[c, k - 1] * active_ref[0, k - 1] > 0, me >= count // 2**k
                )
                raw = raw + jnp.where(usable, 0.0, -1e30).astype(F32)
            logits.append(raw)
        top = functools.reduce(jnp.maximum, [jnp.max(x, axis=0, keepdims=True) for x in logits])
        exps = [jnp.exp(x - top) for x in logits]
        inverse = 1.0 / sum(jnp.sum(x, axis=0, keepdims=True) for x in exps)
        probs = [x * inverse for x in exps]
        weights = [x.astype(BF16) for x in probs]
        prob_grads = [dot(value, grad, ((1,), (1,))) for _, value in pieces]
        delta = sum(
            jnp.sum(w.astype(F32) * x, axis=0, keepdims=True) for w, x in zip(weights, prob_grads)
        )
        query_sum = None
        for k in (1, 3, 2, 0):
            dlogit = (probs[k] * (prob_grads[k] - delta) * scale).astype(BF16)
            key_term = dot(dlogit, query, ((1,), (0,)))
            value_term = dot(weights[k], grad, ((1,), (0,)))
            if k:
                term[k - 1, c, 0] = key_term.astype(BF16)
                term[k - 1, c, 1] = value_term.astype(BF16)
            else:
                own[c, 0] = key_term
                own[c, 1] = value_term
            part = dot(pieces[k][0], dlogit, ((0,), (0,)))
            query_sum = part if query_sum is None else query_sum + part

            if k == 1:

                @pl.when(has_far)
                def _():
                    bwd(0, c, down).start()

            if k == 3:

                @pl.when(odd_or_down)
                def _():
                    bwd(2, c, pair).start()

        dq_ref[:, cols(c)] = query_sum.T.astype(BF16)

    def merge(c):
        @pl.when(has_both)
        def _():
            bwd(0, c, down).wait_recv()

        @pl.when(even_or_down)
        def _():
            bwd(2, c, pair).wait_recv()

        @pl.when(has_down)
        def _():
            for j in range(2):
                side = jnp.where(odd, back[2, c, j].astype(F32), 0.0)
                total = term[1, c, j].astype(F32) + back[0, c, j].astype(F32) + side
                term[1, c, j] = total.astype(BF16)
            bwd(1, c, down).start()

    def finish(c):
        @pl.when(has_up)
        def _():
            bwd(1, c, down).wait_recv()

        for j, out in enumerate((dk_ref, dv_ref)):
            side = jnp.where(even, back[2, c, j].astype(F32), 0.0)
            out[:, cols(c)] = (own[c, j] + back[1, c, j].astype(F32) + side).astype(BF16)

    @pl.loop(0, heads + 2)
    def _(i):
        @pl.when(i + 1 < heads)
        def _():
            forward(i + 1)

        @pl.when(i < heads)
        def _():
            compute(i)

        @pl.when(jnp.logical_and(i >= 1, i <= heads))
        def _():
            merge(i - 1)

        @pl.when(i >= 2)
        def _():
            finish(i - 2)

    for index in range(lanes - 1):
        og_peer(index, lane, twin).wait_send()

    @pl.loop(0, heads)
    def _(c):
        for present, copy in (
            (has_both, fwd(0, kv, c, up)),
            (has_up, fwd(1, kv, c, up)),
            (even_or_down, fwd(2, kv, c, pair)),
            (has_far, bwd(0, c, down)),
            (has_down, bwd(1, c, down)),
            (odd_or_down, bwd(2, c, pair)),
        ):

            @pl.when(present)
            def _():
                copy.wait_send()


def body(count, lanes, queries, key_rows, value_rows, out_grad, out_proj, table, active):
    rows, columns = queries.shape
    heads = columns // HDIM
    block = (heads, 2, rows, HDIM)
    vmem = pl.BlockSpec(memory_space=pltpu.VMEM)
    smem = pl.BlockSpec(memory_space=pltpu.SMEM)
    hbm = pl.BlockSpec(memory_space=pl.ANY)
    dma = pltpu.SemaphoreType.DMA
    return pl.pallas_call(
        functools.partial(kernel, count, lanes),
        out_shape=[jax.ShapeDtypeStruct((rows, columns), BF16)] * 3,
        in_specs=[vmem, hbm, hbm, hbm, hbm, smem, smem],
        out_specs=[vmem] * 3,
        scratch_shapes=[
            pltpu.VMEM(block, BF16),
            pltpu.VMEM((SECTIONS,) + block, BF16),
            pltpu.VMEM((SECTIONS,) + block, BF16),
            pltpu.VMEM((SECTIONS,) + block, BF16),
            pltpu.VMEM(block, F32),
            pltpu.VMEM((lanes,) + out_grad.shape, BF16),
            pltpu.VMEM(out_proj.shape, BF16),
            dma((2, heads)),
            dma((2,)),
            dma((lanes,)),
            dma((lanes,)),
            dma((SECTIONS, heads)),
            dma((SECTIONS, heads)),
            dma((SECTIONS, heads)),
            dma((SECTIONS, heads)),
        ],
        compiler_params=pltpu.CompilerParams(
            collective_id=0, has_side_effects=True, vmem_limit_bytes=60 * 2**20
        ),
    )(queries, key_rows, value_rows, out_grad, out_proj, table, active)


def solution(mesh):
    return jax.shard_map(
        functools.partial(body, mesh.shape["seq"], mesh.shape["head"]),
        mesh=mesh,
        in_specs=(
            P("seq", "head"),
            P("seq", "head"),
            P("seq", "head"),
            P("seq", "head"),
            P("head", None),
            P("head", None),
            P("seq", None),
        ),
        out_specs=(P("seq", "head"), P("seq", "head"), P("seq", "head")),
        check_vma=False,
    )
```

```python
import functools
import math

import jax
import jax.numpy as jnp
from jax import lax
from jax.experimental import pallas as pl
from jax.experimental.pallas import tpu as pltpu
from jax.sharding import PartitionSpec as P

HDIM = 128
SECTIONS = 3
AHEAD = 2
MESH = pl.DeviceIdType.MESH
BF16 = jnp.bfloat16
F32 = jnp.float32


def dot(a, b, dims):
    return lax.dot_general(a, b, (dims, ((), ())), preferred_element_type=F32)


def kernel(
    count,
    lanes,
    q_ref,
    k_hbm,
    v_hbm,
    og_hbm,
    proj_hbm,
    table_ref,
    active_ref,
    dq_ref,
    dk_ref,
    dv_ref,
    kv,
    reach,
    term,
    back,
    own,
    og,
    proj,
    local_sem,
    load_sem,
    og_send,
    og_recv,
    fwd_send,
    fwd_recv,
    bwd_send,
    bwd_recv,
):
    heads, _, rows, _ = kv.shape
    width = og.shape[2]
    scale = 1.0 / math.sqrt(HDIM)
    quarter, eighth = count // 4, count // 8
    me = lax.axis_index("seq")
    lane = lax.axis_index("head")
    odd = (me // eighth) % 2 == 1
    even = jnp.logical_not(odd)
    up, down = me + quarter, me - quarter
    pair = jnp.where(odd, me - eighth, me + eighth)
    has_up, has_down = me < count - quarter, me >= quarter
    has_far = me >= 2 * quarter
    has_both = jnp.logical_and(has_up, has_down)
    odd_or_down = jnp.logical_or(odd, has_down)
    even_or_down = jnp.logical_or(even, has_down)
    twin = jnp.where(lane % 2 == 1, lane - 1, lane + 1)

    def cols(c):
        return pl.ds(pl.multiple_of(c * HDIM, HDIM), HDIM)

    def remote(src, dst, send, recv, axis, target):
        return pltpu.make_async_remote_copy(
            src_ref=src,
            dst_ref=dst,
            send_sem=send,
            recv_sem=recv,
            device_id={axis: target},
            device_id_type=MESH,
        )

    def fwd(kind, src, c, j, target):
        return remote(
            src.at[c, j],
            reach.at[kind, c, j],
            fwd_send.at[kind, j, c],
            fwd_recv.at[kind, j, c],
            "seq",
            target,
        )

    def bwd(kind, c, j, target):
        return remote(
            term.at[kind, c, j],
            back.at[kind, c, j],
            bwd_send.at[kind, j, c],
            bwd_recv.at[kind, j, c],
            "seq",
            target,
        )

    def load_kv(c):
        return [
            pltpu.make_async_copy(src.at[:, cols(c)], kv.at[c, j], local_sem.at[j, c])
            for j, src in enumerate((k_hbm, v_hbm))
        ]

    load_og = pltpu.make_async_copy(og_hbm, og.at[lane], load_sem.at[0])
    load_proj = pltpu.make_async_copy(proj_hbm, proj, load_sem.at[1])
    load_og.start()

    @pl.loop(0, heads)
    def _(c):
        for copy in load_kv(c):
            copy.start()

    load_proj.start()

    barrier = pltpu.get_barrier_semaphore()
    peers = [lax.rem(lane + 2 * j, lanes) for j in range(1, lanes // 2)]
    for peer in [twin] + peers:
        pl.semaphore_signal(barrier, inc=1, device_id={"head": peer}, device_id_type=MESH)
    pl.semaphore_signal(barrier, inc=1, device_id={"seq": pair}, device_id_type=MESH)

    @pl.when(has_up)
    def _():
        pl.semaphore_signal(barrier, inc=1, device_id={"seq": up}, device_id_type=MESH)

    @pl.when(has_down)
    def _():
        pl.semaphore_signal(barrier, inc=1, device_id={"seq": down}, device_id_type=MESH)

    pl.semaphore_wait(
        barrier, 2 + len(peers) + has_up.astype(jnp.int32) + has_down.astype(jnp.int32)
    )

    def send_own(c):
        for j, copy in enumerate(load_kv(c)):
            copy.wait()

            @pl.when(has_up)
            def _():
                fwd(1, kv, c, j, up).start()

            @pl.when(even)
            def _():
                fwd(2, kv, c, j, pair).start()

    def forward(c):
        for j in range(2):

            @pl.when(has_down)
            def _():
                fwd(1, kv, c, j, up).wait_recv()

            @pl.when(has_both)
            def _():
                fwd(0, reach.at[1], c, j, up).start()

            @pl.when(jnp.logical_and(odd, has_down))
            def _():
                fwd(2, reach.at[1], c, j, pair).start()

        @pl.when(c + AHEAD < heads)
        def _():
            send_own(c + AHEAD)

    def og_peer(index, slot, target):
        return remote(
            og.at[slot], og.at[slot], og_send.at[index], og_recv.at[slot], "head", target
        )

    load_og.wait()
    for j, peer in enumerate(peers):
        og_peer(1 + j, lane, peer).start()
    og_peer(0, lane, twin).start()
    for c in range(AHEAD):
        send_own(jnp.int32(c))

    for present, buffer in (
        (has_far, reach.at[0]),
        (has_down, reach.at[1]),
        (odd_or_down, reach.at[2]),
        (has_both, back.at[0]),
        (has_up, back.at[1]),
        (even_or_down, back.at[2]),
    ):

        @pl.when(jnp.logical_not(present))
        def _():
            @pl.loop(0, heads)
            def _(c):
                buffer[c] = jnp.zeros(buffer.shape[1:], BF16)

    forward(jnp.int32(0))
    for j, peer in enumerate(peers):
        og_peer(1 + j, peer, lane).wait_recv()
        og_peer(len(peers) + 1 + j, peer, twin).start()
    load_proj.wait()
    og_peer(0, twin, lane).wait_recv()
    for j in range(len(peers)):
        og_peer(len(peers) + 1 + j, lax.rem(twin + 2 * (j + 1), lanes), lane).wait_recv()

    key_index = lax.broadcasted_iota(jnp.int32, (rows, rows), 0)
    query_index = lax.broadcasted_iota(jnp.int32, (rows, rows), 1)

    def compute(c):
        grad = sum(
            dot(og[p], proj[cols(c), p * width : (p + 1) * width], ((1,), (1,)))
            for p in range(lanes)
        ).astype(BF16)
        query = q_ref[:, cols(c)]

        def key_of(k):
            return reach[k - 1, c, 0] if k else kv[c, 0]

        def logits_of(k):
            raw = dot(key_of(k), query, ((1,), (1,))) * scale
            if k == 0:
                return jnp.where(key_index <= query_index, raw, -1e30)
            usable = jnp.logical_and(
                table_ref[k - 1, c] * active_ref[0, k - 1] > 0, me >= count // 2**k
            )
            return raw + jnp.where(usable, 0.0, -1e30).astype(F32)

        def prob_grad_of(k):
            value = reach[k - 1, c, 1] if k else kv[c, 1]
            return dot(value, grad, ((1,), (1,)))

        logits, prob_grads = {}, {}
        for k in (0, 2):
            logits[k], prob_grads[k] = logits_of(k), prob_grad_of(k)
        for j in range(2):

            @pl.when(odd_or_down)
            def _():
                fwd(2, kv, c, j, pair).wait_recv()

        logits[3], prob_grads[3] = logits_of(3), prob_grad_of(3)
        for j in range(2):

            @pl.when(has_far)
            def _():
                fwd(0, kv, c, j, up).wait_recv()

        logits[1], prob_grads[1] = logits_of(1), prob_grad_of(1)
        sets = range(SECTIONS + 1)
        top = functools.reduce(
            jnp.maximum, [jnp.max(logits[k], axis=0, keepdims=True) for k in sets]
        )
        exps = [jnp.exp(logits[k] - top) for k in sets]
        inverse = 1.0 / sum(jnp.sum(x, axis=0, keepdims=True) for x in exps)
        probs = [x * inverse for x in exps]
        weights = [x.astype(BF16) for x in probs]

        def leave(k, j):
            kind, go = {1: (0, has_far), 3: (2, odd_or_down)}.get(k, (None, None))
            if kind is not None:

                @pl.when(go)
                def _():
                    bwd(kind, c, j, pair if kind == 2 else down).start()

        def keep(k, j, value):
            if k:
                term[k - 1, c, j] = value.astype(BF16)
                leave(k, j)
            else:
                own[c, j] = value

        order = (1, 3, 2, 0)
        for k in order:
            keep(k, 1, dot(weights[k], grad, ((1,), (0,))))
        delta = sum(
            jnp.sum(weights[k].astype(F32) * prob_grads[k], axis=0, keepdims=True) for k in sets
        )
        query_sum = None
        for k in order:
            dlogit = (probs[k] * (prob_grads[k] - delta) * scale).astype(BF16)
            keep(k, 0, dot(dlogit, query, ((1,), (0,))))
            part = dot(key_of(k), dlogit, ((0,), (0,)))
            query_sum = part if query_sum is None else query_sum + part
        dq_ref[:, cols(c)] = query_sum.T.astype(BF16)

    def merge(c):
        for j in (1, 0):

            @pl.when(has_both)
            def _():
                bwd(0, c, j, down).wait_recv()

            @pl.when(even_or_down)
            def _():
                bwd(2, c, j, pair).wait_recv()

            @pl.when(has_down)
            def _():
                side = jnp.where(odd, back[2, c, j].astype(F32), 0.0)
                total = term[1, c, j].astype(F32) + back[0, c, j].astype(F32) + side
                term[1, c, j] = total.astype(BF16)
                bwd(1, c, j, down).start()

    def finish(c):
        for j, out in ((1, dv_ref), (0, dk_ref)):

            @pl.when(has_up)
            def _():
                bwd(1, c, j, down).wait_recv()

            side = jnp.where(even, back[2, c, j].astype(F32), 0.0)
            out[:, cols(c)] = (own[c, j] + back[1, c, j].astype(F32) + side).astype(BF16)

    @pl.loop(0, heads + 2)
    def _(i):
        @pl.when(i + 1 < heads)
        def _():
            forward(i + 1)

        @pl.when(i < heads)
        def _():
            compute(i)

        @pl.when(jnp.logical_and(i >= 1, i <= heads))
        def _():
            merge(i - 1)

        @pl.when(i >= 2)
        def _():
            finish(i - 2)

    for index in range(lanes - 1):
        og_peer(index, lane, twin).wait_send()

    @pl.loop(0, heads)
    def _(c):
        for j in range(2):
            for present, copy in (
                (has_both, fwd(0, kv, c, j, up)),
                (has_up, fwd(1, kv, c, j, up)),
                (even_or_down, fwd(2, kv, c, j, pair)),
                (has_far, bwd(0, c, j, down)),
                (has_down, bwd(1, c, j, down)),
                (odd_or_down, bwd(2, c, j, pair)),
            ):

                @pl.when(present)
                def _():
                    copy.wait_send()


def publish_kernel(parts, *refs):
    number = (len(refs) - 2) // 2
    sources, targets = refs[:number], refs[number : 2 * number]
    held, sems = refs[2 * number :]
    rows = sources[0].shape[0] // parts
    pieces = [(a, p) for a in range(number) for p in range(parts)]

    def fetch(a, p):
        return pltpu.make_async_copy(
            sources[a].at[pl.ds(p * rows, rows)], held.at[a, p], sems.at[0, a, p]
        )

    def store(a, p):
        return pltpu.make_async_copy(
            held.at[a, p], targets[a].at[pl.ds(p * rows, rows)], sems.at[1, a, p]
        )

    for piece in pieces:
        fetch(*piece).start()
    for piece in pieces:
        fetch(*piece).wait()
        store(*piece).start()
    for piece in pieces:
        store(*piece).wait()


def publish(arrays, parts=2):
    rows, columns = arrays[0].shape
    hbm = pl.BlockSpec(memory_space=pl.ANY)
    number = len(arrays)
    return pl.pallas_call(
        functools.partial(publish_kernel, parts),
        out_shape=[jax.ShapeDtypeStruct(a.shape, a.dtype) for a in arrays],
        in_specs=[hbm] * number,
        out_specs=[hbm] * number,
        scratch_shapes=[
            pltpu.VMEM((number, parts, rows // parts, columns), arrays[0].dtype),
            pltpu.SemaphoreType.DMA((2, number, parts)),
        ],
        compiler_params=pltpu.CompilerParams(vmem_limit_bytes=60 * 2**20),
    )(*arrays)


def body(count, lanes, queries, key_rows, value_rows, out_grad, out_proj, table, active):
    rows, columns = queries.shape
    heads = columns // HDIM
    block = (heads, 2, rows, HDIM)
    vmem = pl.BlockSpec(memory_space=pltpu.VMEM)
    smem = pl.BlockSpec(memory_space=pltpu.SMEM)
    hbm = pl.BlockSpec(memory_space=pl.ANY)
    dma = pltpu.SemaphoreType.DMA
    grads = pl.pallas_call(
        functools.partial(kernel, count, lanes),
        out_shape=[jax.ShapeDtypeStruct((rows, columns), BF16)] * 3,
        in_specs=[vmem, hbm, hbm, hbm, hbm, smem, smem],
        out_specs=[vmem] * 3,
        scratch_shapes=[
            pltpu.VMEM(block, BF16),
            pltpu.VMEM((SECTIONS,) + block, BF16),
            pltpu.VMEM((SECTIONS,) + block, BF16),
            pltpu.VMEM((SECTIONS,) + block, BF16),
            pltpu.VMEM(block, F32),
            pltpu.VMEM((lanes,) + out_grad.shape, BF16),
            pltpu.VMEM(out_proj.shape, BF16),
            dma((2, heads)),
            dma((2,)),
            dma((lanes,)),
            dma((lanes,)),
            dma((SECTIONS, 2, heads)),
            dma((SECTIONS, 2, heads)),
            dma((SECTIONS, 2, heads)),
            dma((SECTIONS, 2, heads)),
        ],
        compiler_params=pltpu.CompilerParams(
            collective_id=0, has_side_effects=True, vmem_limit_bytes=60 * 2**20
        ),
    )(queries, key_rows, value_rows, out_grad, out_proj, table.T, active)
    return tuple(publish(grads))


def solution(mesh):
    return jax.shard_map(
        functools.partial(body, mesh.shape["seq"], mesh.shape["head"]),
        mesh=mesh,
        in_specs=(
            P("seq", "head"),
            P("seq", "head"),
            P("seq", "head"),
            P("seq", "head"),
            P("head", None),
            P("head", None),
            P("seq", None),
        ),
        out_specs=(P("seq", "head"), P("seq", "head"), P("seq", "head")),
        check_vma=False,
    )
```

```python
import functools
import math

import jax
import jax.numpy as jnp
from jax import lax
from jax.experimental import pallas as pl
from jax.experimental.pallas import tpu as pltpu
from jax.sharding import PartitionSpec as P

HDIM = 128
SECTIONS = 3
AHEAD = 2
MESH = pl.DeviceIdType.MESH
BF16 = jnp.bfloat16
F32 = jnp.float32


def dot(a, b, dims):
    return lax.dot_general(a, b, (dims, ((), ())), preferred_element_type=F32)


def kernel(
    count,
    lanes,
    q_ref,
    k_hbm,
    v_hbm,
    og_hbm,
    proj_hbm,
    table_ref,
    active_ref,
    dq_hbm,
    dk_hbm,
    dv_hbm,
    kv,
    reach,
    term,
    back,
    own,
    og,
    proj,
    local_sem,
    load_sem,
    og_send,
    og_recv,
    fwd_send,
    fwd_recv,
    bwd_send,
    bwd_recv,
    result,
    out_sem,
):
    heads, _, rows, _ = kv.shape
    width = og.shape[2]
    scale = 1.0 / math.sqrt(HDIM)
    quarter, eighth = count // 4, count // 8
    me = lax.axis_index("seq")
    lane = lax.axis_index("head")
    odd = (me // eighth) % 2 == 1
    even = jnp.logical_not(odd)
    up, down = me + quarter, me - quarter
    pair = jnp.where(odd, me - eighth, me + eighth)
    has_up, has_down = me < count - quarter, me >= quarter
    has_far = me >= 2 * quarter
    has_both = jnp.logical_and(has_up, has_down)
    odd_or_down = jnp.logical_or(odd, has_down)
    even_or_down = jnp.logical_or(even, has_down)
    twin = jnp.where(lane % 2 == 1, lane - 1, lane + 1)

    def cols(c):
        return pl.ds(pl.multiple_of(c * HDIM, HDIM), HDIM)

    def remote(src, dst, send, recv, axis, target):
        return pltpu.make_async_remote_copy(
            src_ref=src,
            dst_ref=dst,
            send_sem=send,
            recv_sem=recv,
            device_id={axis: target},
            device_id_type=MESH,
        )

    def fwd(kind, src, c, j, target):
        return remote(
            src.at[c, j],
            reach.at[kind, c, j],
            fwd_send.at[kind, j, c],
            fwd_recv.at[kind, j, c],
            "seq",
            target,
        )

    def bwd(kind, c, j, target):
        return remote(
            term.at[kind, c, j],
            back.at[kind, c, j],
            bwd_send.at[kind, j, c],
            bwd_recv.at[kind, j, c],
            "seq",
            target,
        )

    def load_kv(c):
        return [
            pltpu.make_async_copy(src.at[:, cols(c)], kv.at[c, j], local_sem.at[j, c])
            for j, src in enumerate((k_hbm, v_hbm))
        ]

    def write(index, c):
        target = (dq_hbm, dk_hbm, dv_hbm)[index]
        return pltpu.make_async_copy(
            result.at[index, c], target.at[:, cols(c)], out_sem.at[index, c]
        )

    load_og = pltpu.make_async_copy(og_hbm, og.at[lane], load_sem.at[0])
    load_proj = pltpu.make_async_copy(proj_hbm, proj, load_sem.at[1])
    load_og.start()

    @pl.loop(0, heads)
    def _(c):
        for copy in load_kv(c):
            copy.start()

    load_proj.start()

    barrier = pltpu.get_barrier_semaphore()
    peers = [lax.rem(lane + 2 * j, lanes) for j in range(1, lanes // 2)]
    for peer in [twin] + peers:
        pl.semaphore_signal(barrier, inc=1, device_id={"head": peer}, device_id_type=MESH)
    pl.semaphore_signal(barrier, inc=1, device_id={"seq": pair}, device_id_type=MESH)

    @pl.when(has_up)
    def _():
        pl.semaphore_signal(barrier, inc=1, device_id={"seq": up}, device_id_type=MESH)

    @pl.when(has_down)
    def _():
        pl.semaphore_signal(barrier, inc=1, device_id={"seq": down}, device_id_type=MESH)

    pl.semaphore_wait(
        barrier, 2 + len(peers) + has_up.astype(jnp.int32) + has_down.astype(jnp.int32)
    )

    def send_own(c):
        for j, copy in enumerate(load_kv(c)):
            copy.wait()

            @pl.when(has_up)
            def _():
                fwd(1, kv, c, j, up).start()

            @pl.when(even)
            def _():
                fwd(2, kv, c, j, pair).start()

    def forward(c):
        for j in range(2):

            @pl.when(has_down)
            def _():
                fwd(1, kv, c, j, up).wait_recv()

            @pl.when(has_both)
            def _():
                fwd(0, reach.at[1], c, j, up).start()

            @pl.when(jnp.logical_and(odd, has_down))
            def _():
                fwd(2, reach.at[1], c, j, pair).start()

        @pl.when(c + AHEAD < heads)
        def _():
            send_own(c + AHEAD)

    def og_peer(index, slot, target):
        return remote(
            og.at[slot], og.at[slot], og_send.at[index], og_recv.at[slot], "head", target
        )

    load_og.wait()
    for j, peer in enumerate(peers):
        og_peer(1 + j, lane, peer).start()
    og_peer(0, lane, twin).start()
    for c in range(AHEAD):
        send_own(jnp.int32(c))

    for present, buffer in (
        (has_far, reach.at[0]),
        (has_down, reach.at[1]),
        (odd_or_down, reach.at[2]),
        (has_both, back.at[0]),
        (has_up, back.at[1]),
        (even_or_down, back.at[2]),
    ):

        @pl.when(jnp.logical_not(present))
        def _():
            @pl.loop(0, heads)
            def _(c):
                buffer[c] = jnp.zeros(buffer.shape[1:], BF16)

    forward(jnp.int32(0))
    for j, peer in enumerate(peers):
        og_peer(1 + j, peer, lane).wait_recv()
        og_peer(len(peers) + 1 + j, peer, twin).start()
    load_proj.wait()
    og_peer(0, twin, lane).wait_recv()
    for j in range(len(peers)):
        og_peer(len(peers) + 1 + j, lax.rem(twin + 2 * (j + 1), lanes), lane).wait_recv()

    key_index = lax.broadcasted_iota(jnp.int32, (rows, rows), 0)
    query_index = lax.broadcasted_iota(jnp.int32, (rows, rows), 1)

    def compute(c):
        grad = sum(
            dot(og[p], proj[cols(c), p * width : (p + 1) * width], ((1,), (1,)))
            for p in range(lanes)
        ).astype(BF16)
        query = q_ref[:, cols(c)]

        def key_of(k):
            return reach[k - 1, c, 0] if k else kv[c, 0]

        def logits_of(k):
            raw = dot(key_of(k), query, ((1,), (1,))) * scale
            if k == 0:
                return jnp.where(key_index <= query_index, raw, -1e30)
            usable = jnp.logical_and(
                table_ref[k - 1, c] * active_ref[0, k - 1] > 0, me >= count // 2**k
            )
            return raw + jnp.where(usable, 0.0, -1e30).astype(F32)

        def prob_grad_of(k):
            value = reach[k - 1, c, 1] if k else kv[c, 1]
            return dot(value, grad, ((1,), (1,)))

        logits, prob_grads = {}, {}
        for k in (0, 2):
            logits[k], prob_grads[k] = logits_of(k), prob_grad_of(k)
        for j in range(2):

            @pl.when(odd_or_down)
            def _():
                fwd(2, kv, c, j, pair).wait_recv()

        logits[3], prob_grads[3] = logits_of(3), prob_grad_of(3)
        for j in range(2):

            @pl.when(has_far)
            def _():
                fwd(0, kv, c, j, up).wait_recv()

        logits[1], prob_grads[1] = logits_of(1), prob_grad_of(1)
        sets = range(SECTIONS + 1)
        top = functools.reduce(
            jnp.maximum, [jnp.max(logits[k], axis=0, keepdims=True) for k in sets]
        )
        exps = [jnp.exp(logits[k] - top) for k in sets]
        inverse = 1.0 / sum(jnp.sum(x, axis=0, keepdims=True) for x in exps)
        probs = [x * inverse for x in exps]
        weights = [x.astype(BF16) for x in probs]

        def leave(k, j):
            kind, go = {1: (0, has_far), 3: (2, odd_or_down)}.get(k, (None, None))
            if kind is not None:

                @pl.when(go)
                def _():
                    bwd(kind, c, j, pair if kind == 2 else down).start()

        def keep(k, j, value):
            if k:
                term[k - 1, c, j] = value.astype(BF16)
                leave(k, j)
            else:
                own[c, j] = value

        order = (1, 3, 2, 0)
        for k in order:
            keep(k, 1, dot(weights[k], grad, ((1,), (0,))))
        delta = sum(
            jnp.sum(weights[k].astype(F32) * prob_grads[k], axis=0, keepdims=True) for k in sets
        )
        query_sum = None
        for k in order:
            dlogit = (probs[k] * (prob_grads[k] - delta) * scale).astype(BF16)
            keep(k, 0, dot(dlogit, query, ((1,), (0,))))
            part = dot(key_of(k), dlogit, ((0,), (0,)))
            query_sum = part if query_sum is None else query_sum + part
        result[0, c] = query_sum.T.astype(BF16)
        write(0, c).start()

    def merge(c):
        for j in (1, 0):

            @pl.when(has_both)
            def _():
                bwd(0, c, j, down).wait_recv()

            @pl.when(even_or_down)
            def _():
                bwd(2, c, j, pair).wait_recv()

            @pl.when(has_down)
            def _():
                side = jnp.where(odd, back[2, c, j].astype(F32), 0.0)
                total = term[1, c, j].astype(F32) + back[0, c, j].astype(F32) + side
                term[1, c, j] = total.astype(BF16)
                bwd(1, c, j, down).start()

    def finish(c):
        for j in (1, 0):

            @pl.when(has_up)
            def _():
                bwd(1, c, j, down).wait_recv()

            side = jnp.where(even, back[2, c, j].astype(F32), 0.0)
            result[1 + j, c] = (own[c, j] + back[1, c, j].astype(F32) + side).astype(BF16)
            write(1 + j, c).start()

    @pl.loop(0, heads + 2)
    def _(i):
        @pl.when(i + 1 < heads)
        def _():
            forward(i + 1)

        @pl.when(i < heads)
        def _():
            compute(i)

        @pl.when(jnp.logical_and(i >= 1, i <= heads))
        def _():
            merge(i - 1)

        @pl.when(i >= 2)
        def _():
            finish(i - 2)

    for index in range(lanes - 1):
        og_peer(index, lane, twin).wait_send()

    @pl.loop(0, heads)
    def _(c):
        for index in range(3):
            write(index, c).wait()
        for j in range(2):
            for present, copy in (
                (has_both, fwd(0, kv, c, j, up)),
                (has_up, fwd(1, kv, c, j, up)),
                (even_or_down, fwd(2, kv, c, j, pair)),
                (has_far, bwd(0, c, j, down)),
                (has_down, bwd(1, c, j, down)),
                (odd_or_down, bwd(2, c, j, pair)),
            ):

                @pl.when(present)
                def _():
                    copy.wait_send()


def publish_kernel(parts, *refs):
    number = (len(refs) - 2) // 2
    sources, targets = refs[:number], refs[number : 2 * number]
    held, sems = refs[2 * number :]
    rows = sources[0].shape[0] // parts
    pieces = [(a, p) for a in range(number) for p in range(parts)]

    def fetch(a, p):
        return pltpu.make_async_copy(
            sources[a].at[pl.ds(p * rows, rows)], held.at[a, p], sems.at[0, a, p]
        )

    def store(a, p):
        return pltpu.make_async_copy(
            held.at[a, p], targets[a].at[pl.ds(p * rows, rows)], sems.at[1, a, p]
        )

    for piece in pieces:
        fetch(*piece).start()
    for piece in pieces:
        fetch(*piece).wait()
        store(*piece).start()
    for piece in pieces:
        store(*piece).wait()


def publish(arrays, parts=2):
    rows, columns = arrays[0].shape
    hbm = pl.BlockSpec(memory_space=pl.ANY)
    number = len(arrays)
    return pl.pallas_call(
        functools.partial(publish_kernel, parts),
        out_shape=[jax.ShapeDtypeStruct(a.shape, a.dtype) for a in arrays],
        in_specs=[hbm] * number,
        out_specs=[hbm] * number,
        scratch_shapes=[
            pltpu.VMEM((number, parts, rows // parts, columns), arrays[0].dtype),
            pltpu.SemaphoreType.DMA((2, number, parts)),
        ],
        compiler_params=pltpu.CompilerParams(vmem_limit_bytes=60 * 2**20),
    )(*arrays)


def body(count, lanes, queries, key_rows, value_rows, out_grad, out_proj, table, active):
    rows, columns = queries.shape
    heads = columns // HDIM
    block = (heads, 2, rows, HDIM)
    vmem = pl.BlockSpec(memory_space=pltpu.VMEM)
    smem = pl.BlockSpec(memory_space=pltpu.SMEM)
    hbm = pl.BlockSpec(memory_space=pl.ANY)
    dma = pltpu.SemaphoreType.DMA
    grads = pl.pallas_call(
        functools.partial(kernel, count, lanes),
        out_shape=[jax.ShapeDtypeStruct((rows, columns), BF16)] * 3,
        in_specs=[vmem, hbm, hbm, hbm, hbm, smem, smem],
        out_specs=[hbm] * 3,
        scratch_shapes=[
            pltpu.VMEM(block, BF16),
            pltpu.VMEM((SECTIONS,) + block, BF16),
            pltpu.VMEM((SECTIONS,) + block, BF16),
            pltpu.VMEM((SECTIONS,) + block, BF16),
            pltpu.VMEM(block, F32),
            pltpu.VMEM((lanes,) + out_grad.shape, BF16),
            pltpu.VMEM(out_proj.shape, BF16),
            dma((2, heads)),
            dma((2,)),
            dma((lanes,)),
            dma((lanes,)),
            dma((SECTIONS, 2, heads)),
            dma((SECTIONS, 2, heads)),
            dma((SECTIONS, 2, heads)),
            dma((SECTIONS, 2, heads)),
            pltpu.VMEM((3, heads, rows, HDIM), BF16),
            dma((3, heads)),
        ],
        compiler_params=pltpu.CompilerParams(
            collective_id=0, has_side_effects=True, vmem_limit_bytes=60 * 2**20
        ),
    )(queries, key_rows, value_rows, out_grad, out_proj, table.T, active)
    return tuple(publish(grads))


def solution(mesh):
    return jax.shard_map(
        functools.partial(body, mesh.shape["seq"], mesh.shape["head"]),
        mesh=mesh,
        in_specs=(
            P("seq", "head"),
            P("seq", "head"),
            P("seq", "head"),
            P("seq", "head"),
            P("head", None),
            P("head", None),
            P("seq", None),
        ),
        out_specs=(P("seq", "head"), P("seq", "head"), P("seq", "head")),
        check_vma=False,
    )
```
